32 devices in a mesh: dp: 4 (over z), ctx: 8 (over y, x, core).
Axes of the slice: x: 2, y: 2, z: 4, core: 2. Of those that a mesh axis runs over, the one named last changes fastest.
Arguments:
- queries: bfloat16 [4, 1024, 4096], P('dp', 'ctx'), may hold values from -120 to 120
- layer_input: bfloat16 [4, 1024, 4096], P('dp', 'ctx'), may hold values from -6 to 6
- key_value_weight: bfloat16 [4096, 1024], P(('dp', 'ctx')), may hold values from -0.25 to 0.25
- output_gradient: bfloat16 [4, 1024, 4096], P('dp', 'ctx'), may hold values from -6 to 6
- document_lengths: int32 [4, 8], P('dp'), may hold values from 1 to 256, 1024 in all within a row
Outputs:
- attended: bfloat16 [4, 1024, 4096], P('dp', 'ctx')
- query_grad: bfloat16 [4, 1024, 4096], P('dp', 'ctx')
- input_grad: bfloat16 [4, 1024, 4096], P('dp', 'ctx')
The draws below stay inside these ranges and needn't reach their ends.
Inputs may be any that keep to these rules, and one draw needn't show every extreme that they name: `document_lengths`: each row holds the lengths of the 8 documents of one sequence in order; they sum to 1024, and one of them is exactly 256.
All inputs are finite; a program needn't handle non-finite values.
Results may differ from the reference program's by a relative error of at most 0.02.
The reference program's roundings to bfloat16 on the way count: a program that leaves them out, or rounds other values in their place, can miss the bound.
Values may be sent and summed in bfloat16 or wider, within the bound.
No kernel may reach another device: no remote copies, remote signals or barrier semaphores. Data moves between devices by JAX's collectives and lax.ppermute only.
A program may use at most 128 MiB of HBM per device.

```python
import math
import jax
import jax.numpy as jnp
import numpy as np
from jax import lax

D = 4096
QUERY_HEADS = 32
KEY_VALUE_HEADS = 4
HEAD_SIZE = 128
TOK_DEV = 128
SEQUENCE_TOKENS = 1024
MAXDOC = 256
NDOC = 8
KVW = 1024
N_DP = 4
N_CTX = 8


def draw_queries(key, part):
    first_key = jax.random.fold_in(key, 11)
    shape = (N_DP, SEQUENCE_TOKENS, QUERY_HEADS * HEAD_SIZE)
    value_rows = jnp.clip(jax.random.normal(first_key, shape, jnp.float32), -6.0, 6.0)
    return value_rows.astype(jnp.bfloat16)


def steps_of(key, shape, pieces, least, high):
    level, own = 1.0, jax.random.fold_in(key, 6)
    for position, blocks in pieces:
        heights = jnp.exp(jax.random.uniform(jax.random.fold_in(own, position), (blocks,), jnp.float32, least / len(pieces), high / len(pieces)))
        level = level * jnp.repeat(heights, shape[position] // blocks).reshape([-1 if axis == position else 1 for axis in range(len(shape))])
    return level


def length_profile(count, total, reach, skew):
    weights = [(1 << 20) // math.isqrt(grade ** skew) + 1 for grade in range(2, count + 1)]
    surplus, holding = total - reach - (count - 1), [1] * (count - 1)
    while surplus > 0:
        free = [i for i in range(count - 1) if holding[i] < reach]
        whole, budget = sum([weights[i] for i in free]), surplus
        for i in free:
            extra = min(reach - holding[i], max(1, budget * weights[i] // whole), surplus)
            holding[i] = holding[i] + extra
            surplus = surplus - extra
    return np.array([reach] + holding)


def uneven(rng, count, total, most, lean):
    if count == 2:
        one = jax.random.randint(rng, (), max(1, total - most), min(most, total - 1) + 1)
        return jnp.stack([one, total - one])
    tallies = jnp.asarray(length_profile(count, total, most, lean), jnp.int32)
    pairs = (count - 1) // 2
    giver, taker = tallies[1:1 + 2 * pairs:2], tallies[2:2 + 2 * pairs:2]
    slack = jnp.minimum(giver - 1, most - taker)
    passed = jax.random.randint(jax.random.fold_in(rng, 1), (pairs,), 0, 1 << 20) % (slack + 1)
    tallies = tallies.at[1:1 + 2 * pairs:2].set(giver - passed).at[2:2 + 2 * pairs:2].set(taker + passed)
    return tallies[jax.random.permutation(jax.random.fold_in(rng, 2), count)]


def scatter_about(key, dims, scale, most, pieces=(), held_as=jnp.bfloat16):
    values = scale * jax.random.normal(key, dims, jnp.float32)
    if pieces:
        values = values * steps_of(key, dims, pieces, -0.22, 0.18)
    return jnp.clip(values, -most, most).astype(held_as)


def setup_inputs(seed: int = 0) -> dict:
    splits = jax.random.split(jax.random.key(seed), 6)
    return {
        "queries": draw_queries(jax.random.fold_in(splits[5], 71), 0),
        "layer_input": scatter_about(splits[1], (N_DP, SEQUENCE_TOKENS, D), 1.0, 6.0, ((0, 4), (1, 8))),
        "key_value_weight": scatter_about(splits[2], (D, KVW), (KVW // 2) ** -0.5, 0.25, ((0, 32),)),
        "output_gradient": scatter_about(splits[3], (N_DP, SEQUENCE_TOKENS, QUERY_HEADS * HEAD_SIZE), 1.0, 6.0, ((0, 4), (1, 8))),
        "document_lengths": jax.vmap(lambda own: uneven(own, NDOC, SEQUENCE_TOKENS, MAXDOC, 2))(jax.random.split(splits[4], N_DP)).reshape((N_DP, NDOC)).astype(jnp.int32),
    }


masked_score = -1e+30

def document_of(positions, ends):
    return lax.optimization_barrier(jnp.sum((positions[..., None] >= ends).astype(jnp.int32), axis=-1))

def reference(queries, layer_input, key_value_weight, output_gradient, document_lengths):
    head_group = QUERY_HEADS // KEY_VALUE_HEADS
    window_reach = N_CTX // 4
    block_slice = TOK_DEV
    window = (window_reach + 1) * block_slice
    half_length = KEY_VALUE_HEADS * HEAD_SIZE
    scale = 1.0 / math.sqrt(HEAD_SIZE)

    def one_sequence(items):
        query_sequence, input_seq, gradient_sequence, lengths = items
        ends = jnp.cumsum(lengths).astype(jnp.int32)
        projected_input = jnp.dot(input_seq, key_value_weight, preferred_element_type=jnp.float32).astype(jnp.bfloat16)
        pad_tokens = jnp.zeros((window_reach * block_slice, KEY_VALUE_HEADS, HEAD_SIZE), jnp.bfloat16)
        key_rows = jnp.concatenate([pad_tokens, projected_input[:, :half_length].reshape(SEQUENCE_TOKENS, KEY_VALUE_HEADS, HEAD_SIZE)], axis=0)
        value_rows = jnp.concatenate([pad_tokens, projected_input[:, half_length:].reshape(SEQUENCE_TOKENS, KEY_VALUE_HEADS, HEAD_SIZE)], axis=0)

        def advance(buffer, index):
            leading = index * block_slice
            query_tile_block = lax.dynamic_slice_in_dim(query_sequence, leading, block_slice, 0).reshape(block_slice, KEY_VALUE_HEADS, head_group, HEAD_SIZE).astype(jnp.float32)
            gradient_block = lax.dynamic_slice_in_dim(gradient_sequence, leading, block_slice, 0).reshape(block_slice, KEY_VALUE_HEADS, head_group, HEAD_SIZE).astype(jnp.float32)
            key_block = lax.dynamic_slice_in_dim(key_rows, leading, window, 0).astype(jnp.float32)
            value_block = lax.dynamic_slice_in_dim(value_rows, leading, window, 0).astype(jnp.float32)
            query_pos = leading + jnp.arange(block_slice, dtype=jnp.int32)
            key_pos = leading - window_reach * block_slice + jnp.arange(window, dtype=jnp.int32)
            allowed = (document_of(query_pos, ends)[:, None] == document_of(key_pos, ends)[None, :]) & (key_pos[None, :] <= query_pos[:, None]) & (key_pos[None, :] >= 0)
            score = scale * jnp.einsum('qhgd,khd->hgqk', query_tile_block, key_block)
            top = lax.optimization_barrier(jnp.max(jnp.where(allowed, score, masked_score), axis=-1))
            weight = jnp.exp(jnp.where(allowed, score - top[..., None], masked_score))
            total = lax.optimization_barrier(jnp.sum(weight, axis=-1))
            mixed = jnp.einsum('hgqk,khd->qhgd', weight.astype(jnp.bfloat16).astype(jnp.float32), value_block)
            output = (mixed / jnp.transpose(total, (2, 0, 1))[..., None]).astype(jnp.bfloat16)
            logsum = top + jnp.log(total)
            product = jnp.transpose(lax.optimization_barrier(jnp.sum(gradient_block * output.astype(jnp.float32), axis=-1)), (1, 2, 0))
            prob = jnp.exp(jnp.where(allowed, score - logsum[..., None], masked_score))
            pressure = jnp.einsum('qhgd,khd->hgqk', gradient_block, value_block)
            slope = (prob * (pressure - product[..., None])).astype(jnp.bfloat16).astype(jnp.float32)
            query_sum = scale * jnp.einsum('hgqk,khd->qhgd', slope, key_block)
            key_part = scale * jnp.einsum('hgqk,qhgd->khd', slope, query_tile_block)
            value_part = jnp.einsum('hgqk,qhgd->khd', prob.astype(jnp.bfloat16).astype(jnp.float32), gradient_block)
            piece = jnp.concatenate([key_part, value_part], axis=-1)
            buffer = lax.dynamic_update_slice_in_dim(buffer, lax.dynamic_slice_in_dim(buffer, leading, window, 0) + piece, leading, 0)
            return (buffer, (output.reshape(block_slice, QUERY_HEADS * HEAD_SIZE), query_sum.astype(jnp.bfloat16).reshape(block_slice, QUERY_HEADS * HEAD_SIZE)))
        start_store = jnp.zeros((SEQUENCE_TOKENS + window_reach * block_slice, KEY_VALUE_HEADS, 2 * HEAD_SIZE), jnp.float32)
        buffer, (outputs, sums) = lax.scan(advance, start_store, jnp.arange(SEQUENCE_TOKENS // block_slice, dtype=jnp.int32))
        outputs = outputs.reshape(SEQUENCE_TOKENS, QUERY_HEADS * HEAD_SIZE)
        sums = sums.reshape(SEQUENCE_TOKENS, QUERY_HEADS * HEAD_SIZE)
        gradient_value = buffer[window_reach * block_slice:].astype(jnp.bfloat16)
        flat = jnp.concatenate([gradient_value[..., :HEAD_SIZE].reshape(SEQUENCE_TOKENS, half_length), gradient_value[..., HEAD_SIZE:].reshape(SEQUENCE_TOKENS, half_length)], axis=1)
        input_grad = jnp.dot(flat, key_value_weight.T, preferred_element_type=jnp.float32).astype(jnp.bfloat16)
        return (outputs, sums, input_grad)
    attended, query_grad, input_grad = lax.map(one_sequence, (queries, layer_input, output_gradient, document_lengths))
    return (attended, query_grad, input_grad)
```

```python
import functools
import math

import jax
import jax.numpy as jnp
from jax import lax
from jax.experimental import pallas as pl
from jax.experimental.pallas import tpu as pltpu
from jax.sharding import PartitionSpec as P

QUERY_HEADS = 32
KEY_VALUE_HEADS = 4
HEAD_SIZE = 128
HEAD_GROUP = QUERY_HEADS // KEY_VALUE_HEADS
HALF = KEY_VALUE_HEADS * HEAD_SIZE
CHUNK_HEADS = 2
CHUNKS = KEY_VALUE_HEADS // CHUNK_HEADS
AXES = ("dp", "ctx")
NEGATIVE = -1e30


VMEM = pl.BlockSpec(memory_space=pltpu.VMEM)
SMEM = pl.BlockSpec(memory_space=pltpu.SMEM)
NT = (((1,), (1,)), ((), ()))


def params():
    return pltpu.CompilerParams(vmem_limit_bytes=48 * 1024 * 1024)


def cost(flops, moved):
    return pl.CostEstimate(flops=flops, bytes_accessed=moved, transcendentals=0)


def columns(index):
    return pl.ds(pl.multiple_of(index * 128, 128), 128)


def project_kernel(last, index_ref, x_ref, *refs):
    refs = list(refs)
    acc_ref = refs.pop(0) if refs[0].dtype == jnp.float32 else None
    pieces, outs = refs[:10], refs[10:]
    rows = jnp.concatenate([x_ref[:, columns(index_ref[j])] for j in range(8)], axis=1)
    for n in range(0, 2 * HALF, 256):
        side = 0 if n < HALF else 1
        cut = slice(n, n + 256)
        part = slice(n - side * HALF, n - side * HALF + 256)
        blocks = [ref[:, cut] for ref in pieces[:6]]
        blocks += [ref[:, part] for ref in pieces[6 + 2 * side : 8 + 2 * side]]
        total = jnp.dot(rows, jnp.concatenate(blocks, axis=0), preferred_element_type=jnp.float32)
        if acc_ref is not None:
            total = total + acc_ref[:, cut]
        if not last:
            outs[0][:, cut] = total
            continue
        value = total.astype(jnp.bfloat16)
        for k in range(0, 256, 128):
            head = (n + k) // HEAD_SIZE - side * KEY_VALUE_HEADS
            place = (side * CHUNK_HEADS + head % CHUNK_HEADS) * HEAD_SIZE
            outs[head // CHUNK_HEADS][:, place : place + 128] = value[:, k : k + 128]


def project(index, x, acc, pieces, last):
    rows = x.shape[0]
    if last:
        out = [jax.ShapeDtypeStruct((rows, 2 * CHUNK_HEADS * HEAD_SIZE), jnp.bfloat16)] * CHUNKS
    else:
        out = [jax.ShapeDtypeStruct((rows, 2 * HALF), jnp.float32)]
    given = [x] + ([] if acc is None else [acc]) + list(pieces)
    return pl.pallas_call(
        functools.partial(project_kernel, last),
        out_shape=out,
        in_specs=[SMEM] + [VMEM] * len(given),
        out_specs=[VMEM] * len(out),
        compiler_params=params(),
        cost_estimate=cost(2 * rows * 1024 * 2 * HALF, 4 << 20),
        name="project",
    )(index, *given)


def attend_kernel(blocks, chunk, reach, start_ref, lengths_ref, q_ref, g_ref, *refs):
    refs = list(refs)
    kv = [refs.pop(0) for _ in range(reach + 1)]
    if chunk:
        refs.pop(0)
        refs.pop(0)
    o_ref, dq_ref = refs[0], refs[1]
    parts = refs[2 : 3 + reach]
    bias_ref, p_ref, s_ref = refs[3 + reach :]
    rows = q_ref.shape[0]
    window = (reach + 1) * rows
    start = start_ref[0]
    key_pos = start - reach * rows + lax.broadcasted_iota(jnp.int32, (window, rows), 0)
    query_pos = start + lax.broadcasted_iota(jnp.int32, (8, rows), 1)
    key_doc = jnp.zeros((window, rows), jnp.int32)
    query_doc = jnp.zeros((8, rows), jnp.int32)
    end = jnp.int32(0)
    for document in range(lengths_ref.shape[1]):
        end = end + lengths_ref[0, document]
        key_doc = key_doc + (key_pos >= end).astype(jnp.int32)
        query_doc = query_doc + (query_pos >= end).astype(jnp.int32)
    allowed = (key_doc == query_doc[:1]) & (key_pos <= query_pos[:1]) & (key_pos >= 0)
    bias = jnp.where(allowed, 0.0, NEGATIVE)
    bias_ref[:, :rows] = bias
    bias_ref[:, rows:] = bias
    scale = 1.0 / math.sqrt(HEAD_SIZE)
    factor = scale * math.log2(math.e)
    for head in range(CHUNK_HEADS):
        k_cut = slice(head * HEAD_SIZE, (head + 1) * HEAD_SIZE)
        v_cut = slice((CHUNK_HEADS + head) * HEAD_SIZE, (CHUNK_HEADS + head + 1) * HEAD_SIZE)
        keys = jnp.concatenate([kv[reach - j][:, k_cut] for j in range(reach + 1)], axis=0)
        values = jnp.concatenate([kv[reach - j][:, v_cut] for j in range(reach + 1)], axis=0)
        keys_t = keys.T
        values_t = values.T
        base = head * HEAD_GROUP * HEAD_SIZE
        for pair in range(0, HEAD_GROUP, 2):
            cuts = [slice(base + (pair + j) * HEAD_SIZE, base + (pair + j + 1) * HEAD_SIZE) for j in range(2)]
            spot = slice(pair * rows, (pair + 2) * rows)
            q = jnp.concatenate([q_ref[:, cut] for cut in cuts], axis=0)
            g = jnp.concatenate([g_ref[:, cut] for cut in cuts], axis=0)
            score = lax.dot_general(keys, q, NT, preferred_element_type=jnp.float32) + bias_ref[...]
            top = jnp.max(score, axis=0, keepdims=True)
            weight = jnp.exp2((score - top) * factor)
            inverse = 1.0 / jnp.sum(weight, axis=0, keepdims=True)
            mixed = jnp.dot(values_t, weight.astype(jnp.bfloat16), preferred_element_type=jnp.float32)
            mixed = (mixed * inverse).astype(jnp.bfloat16)
            prob = weight * inverse
            pressure = lax.dot_general(values, g, NT, preferred_element_type=jnp.float32)
            product = jnp.sum(prob * pressure, axis=0, keepdims=True)
            slope = (prob * (pressure - product)).astype(jnp.bfloat16)
            p_ref[:, spot] = prob.astype(jnp.bfloat16)
            s_ref[:, spot] = slope
            dq = jnp.dot(keys_t, slope, preferred_element_type=jnp.float32)
            dq = (dq * scale).astype(jnp.bfloat16)
            for j, cut in enumerate(cuts):
                o_ref[:, cut] = mixed[:, j * rows : (j + 1) * rows].T
                dq_ref[:, cut] = dq[:, j * rows : (j + 1) * rows].T
        heads = [slice(base + j * HEAD_SIZE, base + (j + 1) * HEAD_SIZE) for j in range(HEAD_GROUP)]
        q_all = jnp.concatenate([q_ref[:, cut] for cut in heads], axis=0)
        g_all = jnp.concatenate([g_ref[:, cut] for cut in heads], axis=0)
        for j in range(reach + 1):
            span = slice((reach - j) * rows, (reach - j + 1) * rows)
            dk = jnp.dot(s_ref[span, :], q_all, preferred_element_type=jnp.float32) * scale
            dv = jnp.dot(p_ref[span, :], g_all, preferred_element_type=jnp.float32)
            parts[j][:, k_cut] = dk.astype(parts[j].dtype)
            parts[j][:, v_cut] = dv.astype(parts[j].dtype)


def attend(start, lengths, queries, gradient, kv, chunk, filled):
    rows, width = queries.shape
    reach = len(kv) - 1
    share = width // CHUNKS
    window = (reach + 1) * rows
    wide = pl.BlockSpec((rows, share), lambda i: (0, chunk))
    part = pl.BlockSpec((rows, 2 * CHUNK_HEADS * HEAD_SIZE), lambda i: (0, 0))
    given = [start, lengths, queries, gradient, *kv] + ([] if chunk == 0 else list(filled))
    aliases = {} if chunk == 0 else {5 + reach: 0, 6 + reach: 1}
    whole = jax.ShapeDtypeStruct((rows, width), jnp.bfloat16)
    piece = (rows, 2 * CHUNK_HEADS * HEAD_SIZE)
    outs = pl.pallas_call(
        functools.partial(attend_kernel, None, chunk, reach),
        grid=(1,),
        out_shape=[whole, whole]
        + [jax.ShapeDtypeStruct(piece, jnp.float32 if j == 0 else jnp.bfloat16) for j in range(reach + 1)],
        in_specs=[SMEM, SMEM, wide, wide]
        + [part] * (reach + 1)
        + ([] if chunk == 0 else [pl.BlockSpec(memory_space=pl.ANY)] * 2),
        out_specs=[wide, wide] + [part] * (reach + 1),
        scratch_shapes=[
            pltpu.VMEM((window, 2 * rows), jnp.float32),
            pltpu.VMEM((window, HEAD_GROUP * rows), jnp.bfloat16),
            pltpu.VMEM((window, HEAD_GROUP * rows), jnp.bfloat16),
        ],
        input_output_aliases=aliases,
        compiler_params=params(),
        cost_estimate=cost(12 * rows * window * share * 2, 4 << 20),
        name="attend",
    )(*given)
    return outs[:2], outs[2:]


def finish_kernel(slots, reach, index_ref, *refs):
    refs = list(refs)
    parts = [[refs.pop(0) for _ in range(reach + 1)] for _ in range(CHUNKS)]
    pieces = [[refs.pop(0) for _ in range(10)] for _ in range(slots)]
    out_ref, flat_ref = refs
    cut = CHUNK_HEADS * HEAD_SIZE
    for chunk in range(CHUNKS):
        total = parts[chunk][0][...]
        for ref in parts[chunk][1:]:
            total = total + ref[...].astype(jnp.float32)
        total = total.astype(jnp.bfloat16)
        flat_ref[:, chunk * cut : (chunk + 1) * cut] = total[:, :cut]
        flat_ref[:, HALF + chunk * cut : HALF + (chunk + 1) * cut] = total[:, cut:]
    flat = flat_ref[...]
    for slot in range(slots):
        for j in range(4):
            if j < 3:
                mine = jnp.concatenate([ref[...] for ref in pieces[slot][2 * j : 2 * j + 2]], axis=0)
                total = lax.dot_general(flat, mine, NT, preferred_element_type=jnp.float32)
            else:
                total = 0.0
                for side in range(2):
                    mine = jnp.concatenate([ref[...] for ref in pieces[slot][6 + 2 * side : 8 + 2 * side]], axis=0)
                    total = total + lax.dot_general(
                        flat[:, side * HALF : (side + 1) * HALF], mine, NT, preferred_element_type=jnp.float32
                    )
            value = total.astype(jnp.bfloat16)
            for side in range(2):
                place = columns(index_ref[8 * slot + 2 * j + side])
                out_ref[:, place] = value[:, side * 128 : (side + 1) * 128]


def finish(index, parts, pieces, width):
    rows = parts[0][0].shape[0]
    reach = len(parts[0]) - 1
    given = [p for group in parts for p in group] + [p for group in pieces for p in group]
    return pl.pallas_call(
        functools.partial(finish_kernel, len(pieces), reach),
        out_shape=jax.ShapeDtypeStruct((rows, width), jnp.bfloat16),
        in_specs=[SMEM] + [VMEM] * len(given),
        out_specs=VMEM,
        scratch_shapes=[pltpu.VMEM((rows, 2 * HALF), jnp.bfloat16)],
        compiler_params=params(),
        cost_estimate=cost(2 * rows * width * 2 * HALF, 10 << 20),
        name="finish",
    )(index, *given)


def shards(sizes, queries, layer_input, key_value_weight, output_gradient, document_lengths):
    depth, across = sizes
    inputs = layer_input[0]
    rows = inputs.shape[0]
    width = inputs.shape[1]
    z = lax.axis_index("dp")
    place = lax.axis_index("ctx")
    reach = across // 4
    start = (place * rows).astype(jnp.int32).reshape(1)

    def moved(value, target):
        pairs = []
        for a in range(depth):
            for b in range(across):
                to = target(a, b)
                if to is not None:
                    pairs.append((a * across + b, to[0] * across + to[1]))
        return lax.ppermute(value, AXES, pairs)

    def over_x(value):
        return moved(value, lambda a, b: (a, b ^ 2))

    def over_y(value):
        return moved(value, lambda a, b: (a, b ^ 4))

    def over_core(value):
        return moved(value, lambda a, b: (a, b ^ 1))

    def up(value):
        return moved(value, lambda a, b: ((a + 1) % depth, b))

    def behind(value, steps):
        return moved(value, lambda a, b: (a, b + steps) if 0 <= b + steps < across else None)

    by_hand = across == 8 and key_value_weight.shape[0] == 128
    if by_hand:
        held = key_value_weight
        slots, acc, index = [], None, []
        for slot in range(depth):
            after = up(held) if slot + 1 < depth else None
            rx, ry = over_x(held), over_y(held)
            dk, dv = over_y(rx[:, :HALF]), over_x(ry[:, HALF:])
            mine = [held, rx, ry, dk, dv]
            pieces = []
            for piece in mine:
                pieces += [piece, over_core(piece)]
            slots.append(pieces)
            base = ((z + depth - slot) % depth) * across
            order = []
            for flip in (0, 2, 4, 6):
                order += [base + (place ^ flip), base + (place ^ flip ^ 1)]
            index.append(jnp.stack(order).astype(jnp.int32))
            acc = project(index[-1], inputs, acc, pieces, slot + 1 == depth)
            if slot + 1 < depth:
                acc = acc[0]
            held = after
        chunks = acc
    else:
        full = lax.all_gather(key_value_weight, AXES, axis=0, tiled=True)
        flat = jnp.dot(inputs, full, preferred_element_type=jnp.float32).astype(jnp.bfloat16)
        cut = CHUNK_HEADS * HEAD_SIZE
        chunks = [
            jnp.concatenate([flat[:, c * cut : (c + 1) * cut], flat[:, HALF + c * cut : HALF + (c + 1) * cut]], axis=1)
            for c in range(CHUNKS)
        ]
    kvs = [[chunk] + [behind(chunk, step) for step in range(1, reach + 1)] for chunk in chunks]
    filled, parts = None, []
    for chunk in range(CHUNKS):
        filled, pieces = attend(
            start, document_lengths, queries[0], output_gradient[0], kvs[chunk], chunk, filled
        )
        parts.append([pieces[0]] + [behind(pieces[step], -step) for step in range(1, reach + 1)])
    if by_hand:
        input_grad = finish(jnp.concatenate(index), parts, slots, width)
    else:
        sums = []
        for group in parts:
            total = group[0]
            for piece in group[1:]:
                total = total + piece.astype(jnp.float32)
            sums.append(total.astype(jnp.bfloat16))
        cut = CHUNK_HEADS * HEAD_SIZE
        flat = jnp.concatenate([s[:, :cut] for s in sums] + [s[:, cut:] for s in sums], axis=1)
        input_grad = lax.dot_general(flat, full, NT, preferred_element_type=jnp.float32).astype(jnp.bfloat16)
    return (filled[0][None], filled[1][None], input_grad[None])


def solution(mesh):
    sizes = (mesh.shape["dp"], mesh.shape["ctx"])
    return jax.shard_map(
        functools.partial(shards, sizes),
        mesh=mesh,
        in_specs=(
            P("dp", "ctx", None),
            P("dp", "ctx", None),
            P(("dp", "ctx"), None),
            P("dp", "ctx", None),
            P("dp", None),
        ),
        out_specs=(P("dp", "ctx", None), P("dp", "ctx", None), P("dp", "ctx", None)),
        check_vma=False,
    )
```

```python
import functools
import math

import jax
import jax.numpy as jnp
from jax import lax
from jax.experimental import pallas as pl
from jax.experimental.pallas import tpu as pltpu
from jax.sharding import PartitionSpec as P


QUERY_HEADS = 32
KEY_VALUE_HEADS = 4
HEAD_SIZE = 128
HEAD_GROUP = QUERY_HEADS // KEY_VALUE_HEADS
HALF = KEY_VALUE_HEADS * HEAD_SIZE
CHUNK_HEADS = 2
CHUNKS = KEY_VALUE_HEADS // CHUNK_HEADS
AXES = ("dp", "ctx")
NEGATIVE = -1e30


VMEM = pl.BlockSpec(memory_space=pltpu.VMEM)
SMEM = pl.BlockSpec(memory_space=pltpu.SMEM)
HBM = pl.BlockSpec(memory_space=pltpu.HBM)
NT = (((1,), (1,)), ((), ()))


def params(mib):
    return pltpu.CompilerParams(vmem_limit_bytes=mib * 1024 * 1024)


def cost(flops, moved):
    return pl.CostEstimate(flops=flops, bytes_accessed=moved, transcendentals=0)


def inside(value):
    return pltpu.with_memory_space_constraint(value, pltpu.VMEM)


def outside(value):
    return pltpu.with_memory_space_constraint(value, pltpu.HBM)


def columns(index):
    return pl.ds(pl.multiple_of(index * 128, 128), 128)


def shard_of(depth, across, core, block):
    z = lax.axis_index("dp")
    place = lax.axis_index("ctx")
    source = z - block // 4
    source = jnp.where(source < 0, source + depth, source)
    place = place - 2 * (place % 2) * core + core
    flip = block % 4
    if flip & 1:
        place = place + 2 - 4 * ((place // 2) % 2)
    if flip & 2:
        place = place + 4 - 8 * ((place // 4) % 2)
    return source * across + place


def arrange_kernel(sizes, x_ref, y_ref, out_ref):
    rows = x_ref.shape[0]
    for j in range(out_ref.shape[1] // 128):
        place = slice(j * 128, (j + 1) * 128)
        shard = shard_of(*sizes, 0, j)
        out_ref[:rows, place] = x_ref[:, columns(shard)]
        out_ref[rows:, place] = y_ref[:, columns(shard)]


def arrange(sizes, mine, other):
    rows, width = mine.shape
    return pl.pallas_call(
        functools.partial(arrange_kernel, sizes),
        out_shape=pltpu.VMEM((2 * rows, width // 2), mine.dtype),
        in_specs=[VMEM, VMEM],
        out_specs=VMEM,
        compiler_params=params(16),
        cost_estimate=cost(1 << 20, 3 << 20),
        name="arrange",
    )(mine, inside(other))


def fetch_kernel(count, *refs):
    sems = refs[-1]
    moves = [pltpu.make_async_copy(refs[j], refs[count + j], sems.at[j]) for j in range(count)]
    for move in moves:
        move.start()
    for move in moves:
        move.wait()


def fetch(*values):
    count = len(values)
    return pl.pallas_call(
        functools.partial(fetch_kernel, count),
        out_shape=[pltpu.VMEM(value.shape, value.dtype) for value in values],
        in_specs=[HBM] * count,
        out_specs=[VMEM] * count,
        scratch_shapes=[pltpu.SemaphoreType.DMA((count,))],
        compiler_params=params(16),
        cost_estimate=cost(1 << 20, 4 << 20),
        name="fetch",
    )(*[outside(value) for value in values])


def project_kernel(slot, count, last, x_ref, *refs):
    refs = list(refs)
    if slot:
        acc_ref = refs.pop(0)
    pieces = [refs.pop(0) for _ in range(count)]
    packed_ref = refs.pop(0)
    outs = refs
    rows = x_ref[:, slice(slot * 512, (slot + 1) * 512)]
    half = rows.shape[0] // 2
    for n in range(0, 2 * HALF, 256):
        side = 0 if n < HALF else 1
        cut = slice(n, n + 256)
        part = slice(n - side * HALF, n - side * HALF + 256)
        blocks = [ref[:, cut] for ref in pieces[:3]]
        blocks.append(pieces[3][:, cut] if count == 4 else pieces[3 + side][:, part])
        weight = jnp.concatenate(blocks, axis=0)
        packed_ref[:, cut] = weight
        total = jnp.dot(rows, weight, preferred_element_type=jnp.float32)
        if slot:
            total = total + acc_ref[:, cut]
        if last:
            outs[0][:, cut] = total[:half]
            outs[1][:, cut] = total[half:]
        else:
            outs[0][:, cut] = total


def project(slot, x, acc, pieces, last):
    rows = x.shape[0] // 2
    out = [pltpu.VMEM((rows, 2 * HALF), jnp.float32)] * 2
    if not last:
        out = [pltpu.VMEM((2 * rows, 2 * HALF), jnp.float32)]
    given = [inside(x)] + ([] if slot == 0 else [inside(acc)])
    given += list(pieces[:1] if slot == 0 else []) + [inside(piece) for piece in pieces[0 if slot else 1 :]]
    outs = pl.pallas_call(
        functools.partial(project_kernel, slot, len(pieces), last),
        out_shape=[pltpu.VMEM((512, 2 * HALF), jnp.bfloat16)] + out,
        in_specs=[VMEM] * len(given),
        out_specs=[VMEM] * (len(out) + 1),
        compiler_params=params(16),
        cost_estimate=cost(4 * rows * 512 * 2 * HALF, 4 << 20),
        name="project",
    )(*given)
    return outs[0], outs[1:]


def join_kernel(a_ref, b_ref, *outs):
    cut = CHUNK_HEADS * HEAD_SIZE
    for c, out in enumerate(outs):
        for side in range(2):
            span = slice(side * HALF + c * cut, side * HALF + (c + 1) * cut)
            out[:, side * cut : (side + 1) * cut] = (a_ref[:, span] + b_ref[:, span]).astype(out.dtype)


def join(mine, other):
    rows = mine.shape[0]
    return pl.pallas_call(
        join_kernel,
        out_shape=[pltpu.VMEM((rows, 2 * CHUNK_HEADS * HEAD_SIZE), jnp.bfloat16)] * CHUNKS,
        in_specs=[VMEM, VMEM],
        out_specs=[VMEM] * CHUNKS,
        compiler_params=params(16),
        cost_estimate=cost(1 << 20, 2 << 20),
        name="join",
    )(inside(mine), inside(other))


def attend_kernel(chunk, reach, lengths_ref, q_ref, g_ref, *refs):
    refs = list(refs)
    kv = [refs.pop(0) for _ in range(reach + 1)]
    o_ref, dq_ref = refs[0], refs[1]
    parts = refs[2 : 3 + reach]
    bias_ref, score_ref, press_ref, w_ref, p_ref, s_ref = refs[3 + reach :]
    rows = q_ref.shape[0]
    share = o_ref.shape[1]
    window = (reach + 1) * rows
    start = lax.axis_index("ctx") * rows
    key_pos = start - reach * rows + lax.broadcasted_iota(jnp.int32, (window, rows), 0)
    query_pos = start + lax.broadcasted_iota(jnp.int32, (8, rows), 1)
    key_doc = jnp.zeros((window, rows), jnp.int32)
    query_doc = jnp.zeros((8, rows), jnp.int32)
    end = jnp.int32(0)
    for document in range(lengths_ref.shape[1]):
        end = end + lengths_ref[0, document]
        key_doc = key_doc + (key_pos >= end).astype(jnp.int32)
        query_doc = query_doc + (query_pos >= end).astype(jnp.int32)
    allowed = (key_doc == query_doc[:1]) & (key_pos <= query_pos[:1]) & (key_pos >= 0)
    bias_ref[...] = jnp.where(allowed, 0.0, NEGATIVE)
    scale = 1.0 / math.sqrt(HEAD_SIZE)
    factor = scale * math.log2(math.e)
    size = HEAD_GROUP * rows
    for head in range(CHUNK_HEADS):
        k_cut = slice(head * HEAD_SIZE, (head + 1) * HEAD_SIZE)
        v_cut = slice((CHUNK_HEADS + head) * HEAD_SIZE, (CHUNK_HEADS + head + 1) * HEAD_SIZE)
        keys = jnp.concatenate([kv[reach - j][:, k_cut] for j in range(reach + 1)], axis=0)
        values = jnp.concatenate([kv[reach - j][:, v_cut] for j in range(reach + 1)], axis=0)
        keys_t = keys.T
        values_t = values.T
        base = head * HEAD_GROUP * HEAD_SIZE
        outs = [slice(base + j * HEAD_SIZE, base + (j + 1) * HEAD_SIZE) for j in range(HEAD_GROUP)]
        cuts = [slice(cut.start + chunk * share, cut.stop + chunk * share) for cut in outs]
        mine = slice(head * size, (head + 1) * size)
        q_all = jnp.concatenate([q_ref[:, cut] for cut in cuts], axis=0)
        g_all = jnp.concatenate([g_ref[:, cut] for cut in cuts], axis=0)
        score_ref[:, mine] = lax.dot_general(keys, q_all, NT, preferred_element_type=jnp.float32)
        press_ref[:, mine] = lax.dot_general(values, g_all, NT, preferred_element_type=jnp.float32)
        inverses = []
        for j in range(HEAD_GROUP):
            spot = slice(head * size + j * rows, head * size + (j + 1) * rows)
            score = score_ref[:, spot] + bias_ref[...]
            top = jnp.max(score, axis=0, keepdims=True)
            weight = jnp.exp2((score - top) * factor)
            inverse = 1.0 / jnp.sum(weight, axis=0, keepdims=True)
            inverses.append(inverse)
            w_ref[:, spot] = weight.astype(jnp.bfloat16)
            prob = weight * inverse
            p_ref[:, spot] = prob.astype(jnp.bfloat16)
            product = jnp.sum(prob * press_ref[:, spot], axis=0, keepdims=True)
            s_ref[:, spot] = (prob * (press_ref[:, spot] - product)).astype(jnp.bfloat16)
        mixed = jnp.dot(values_t, w_ref[:, mine], preferred_element_type=jnp.float32)
        mixed = (mixed * jnp.concatenate(inverses, axis=1)).astype(jnp.bfloat16)
        dq = jnp.dot(keys_t, s_ref[:, mine], preferred_element_type=jnp.float32)
        dq = (dq * scale).astype(jnp.bfloat16)
        for j, cut in enumerate(outs):
            o_ref[:, cut] = mixed[:, j * rows : (j + 1) * rows].T
            dq_ref[:, cut] = dq[:, j * rows : (j + 1) * rows].T
        for j in range(reach + 1):
            span = slice((reach - j) * rows, (reach - j + 1) * rows)
            dk = jnp.dot(s_ref[span, mine], q_all, preferred_element_type=jnp.float32) * scale
            dv = jnp.dot(p_ref[span, mine], g_all, preferred_element_type=jnp.float32)
            parts[j][:, k_cut] = dk.astype(parts[j].dtype)
            parts[j][:, v_cut] = dv.astype(parts[j].dtype)


def attend(lengths, queries, gradient, kv, chunk):
    rows, width = queries.shape
    reach = len(kv) - 1
    share = width // CHUNKS
    window = (reach + 1) * rows
    given = [lengths] + [inside(value) for value in (queries, gradient, *kv)]
    whole = pltpu.VMEM((rows, share), jnp.bfloat16)
    piece = (rows, 2 * CHUNK_HEADS * HEAD_SIZE)
    size = CHUNK_HEADS * HEAD_GROUP * rows
    outs = pl.pallas_call(
        functools.partial(attend_kernel, chunk, reach),
        out_shape=[whole, whole]
        + [pltpu.VMEM(piece, jnp.float32 if j == 0 else jnp.bfloat16) for j in range(reach + 1)],
        in_specs=[SMEM] + [VMEM] * (reach + 3),
        out_specs=[VMEM] * (reach + 3),
        scratch_shapes=[
            pltpu.VMEM((window, rows), jnp.float32),
            pltpu.VMEM((window, size), jnp.float32),
            pltpu.VMEM((window, size), jnp.float32),
            pltpu.VMEM((window, size), jnp.bfloat16),
            pltpu.VMEM((window, size), jnp.bfloat16),
            pltpu.VMEM((window, size), jnp.bfloat16),
        ],
        compiler_params=params(min(60, 14 + 14 * window * size // (1 << 20))),
        cost_estimate=cost(12 * rows * window * share * 2, 4 << 20),
        name="attend",
    )(*given)
    return outs[:2], outs[2:]


def finish_kernel(sizes, chunk, terms, slots, extra, *refs):
    refs = list(refs)
    parts = [refs.pop(0) for _ in range(terms)]
    if chunk:
        acc_ref = refs.pop(0)
    halves = [[refs.pop(0) for _ in range(slots)] for _ in range(2)]
    results = [refs.pop(0) for _ in range(extra)]
    out_ref = refs.pop(0)
    last = chunk + 1 == CHUNKS
    moves = []
    if extra:
        sems = refs.pop()
        for j, ref in enumerate(results):
            share = ref.shape[1]
            spot = slice((j // 2) * share, (j // 2 + 1) * share)
            moves.append(pltpu.make_async_copy(ref, refs[j % 2].at[:, spot], sems.at[j]))
            moves[-1].start()
    if last:
        staged_ref, out_sems = refs
    cut = CHUNK_HEADS * HEAD_SIZE
    total = parts[0][...]
    for part in parts[1:]:
        total = total + part[...].astype(jnp.float32)
    flat = total.astype(jnp.bfloat16)
    near_cut = slice(chunk * cut, (chunk + 1) * cut)
    far_cut = slice(HALF + chunk * cut, HALF + (chunk + 1) * cut)
    for block in range(4 * slots):
        span = slice((block % 4) * 128, (block % 4 + 1) * 128)
        pair = [half[block // 4] for half in halves]
        weight = jnp.concatenate([ref[span, near_cut] for ref in pair], axis=0)
        result = lax.dot_general(flat[:, :cut], weight, NT, preferred_element_type=jnp.float32)
        weight = jnp.concatenate([ref[span, far_cut] for ref in pair], axis=0)
        result = result + lax.dot_general(flat[:, cut:], weight, NT, preferred_element_type=jnp.float32)
        near = slice(block * 256, (block + 1) * 256)
        if chunk:
            result = result + acc_ref[:, near]
        if not last:
            out_ref[:, near] = result
            continue
        staged_ref[:, near] = result.astype(jnp.bfloat16)
        for core in range(2):
            shard = shard_of(*sizes, core, block)
            moves.append(
                pltpu.make_async_copy(
                    staged_ref.at[:, slice(block * 256 + core * 128, block * 256 + (core + 1) * 128)],
                    out_ref.at[:, columns(shard)],
                    out_sems.at[2 * block + core],
                )
            )
            moves[-1].start()
    for move in moves:
        move.wait()


def finish(sizes, chunk, parts, acc, halves, results):
    rows = parts[0].shape[0]
    slots = len(halves) // 2
    width = len(halves) * 512
    given = [inside(value) for value in list(parts) + ([acc] if chunk else []) + list(halves) + list(results)]
    out, specs = [pltpu.VMEM((rows, width), jnp.float32)], [VMEM]
    scratch = []
    if results:
        out += [pltpu.HBM((rows, width), jnp.bfloat16)] * 2
        specs += [HBM] * 2
        scratch = [pltpu.SemaphoreType.DMA((len(results),))]
    if chunk + 1 == CHUNKS:
        out[0], specs[0] = pltpu.HBM((rows, width), jnp.bfloat16), HBM
        scratch += [pltpu.VMEM((rows, width), jnp.bfloat16), pltpu.SemaphoreType.DMA((8 * slots,))]
    return pl.pallas_call(
        functools.partial(finish_kernel, sizes, chunk, len(parts), slots, len(results)),
        out_shape=out,
        in_specs=[VMEM] * len(given),
        out_specs=specs,
        scratch_shapes=scratch,
        compiler_params=params(16),
        cost_estimate=cost(2 * rows * width * 2 * HALF // CHUNKS, 10 << 20),
        name="finish",
    )(*given)


def halved(slot, depth):
    return slot == 0 or slot == depth - 1 or depth % 2 == 1


def shards(sizes, queries, layer_input, key_value_weight, output_gradient, document_lengths):
    depth, across = sizes
    inputs = layer_input[0]
    reach = across // 4

    queries, gradient = queries[0], output_gradient[0]

    def moved(value, target):
        pairs = []
        for a in range(depth):
            for b in range(across):
                to = target(a, b)
                if to is not None:
                    pairs.append((a * across + b, to[0] * across + to[1]))
        return lax.ppermute(value, AXES, pairs)

    def over_x(value):
        return moved(value, lambda a, b: (a, b ^ 2))

    def over_y(value):
        return moved(value, lambda a, b: (a, b ^ 4))

    def over_core(value):
        return moved(value, lambda a, b: (a, b ^ 1))

    def along(value, steps):
        return moved(value, lambda a, b: ((a + steps) % depth, b))

    def behind(value, steps):
        return moved(value, lambda a, b: (a, b + steps) if 0 <= b + steps < across else None)

    by_hand = across == 8 and key_value_weight.shape[0] == 128
    if by_hand:
        held = key_value_weight
        acc, mine, theirs = None, [], []
        other = over_core(inputs)
        queries, gradient = fetch(queries, gradient)
        lined = arrange(sizes, inputs, other)
        for slot in range(depth):
            after = along(held, 1) if slot + 1 < depth else None
            rx, ry = over_x(held), over_y(held)
            pieces = [held, rx, ry]
            if halved(slot, depth):
                pieces += [over_y(rx[:, :HALF]), over_x(ry[:, HALF:])]
            elif slot % 2:
                pieces += [over_y(rx)]
            else:
                pieces += [over_x(ry)]
            packed, acc = project(slot, lined, acc, pieces, slot + 1 == depth)
            mine.append(packed)
            theirs.append(over_core(packed))
            if slot + 1 < depth:
                acc = acc[0]
            held = after
        got = over_core(acc[1])
        chunks = join(acc[0], got)
    else:
        full = lax.all_gather(key_value_weight, AXES, axis=0, tiled=True)
        flat = jnp.dot(inputs, full, preferred_element_type=jnp.float32).astype(jnp.bfloat16)
        cut = CHUNK_HEADS * HEAD_SIZE
        chunks = [
            jnp.concatenate([flat[:, c * cut : (c + 1) * cut], flat[:, HALF + c * cut : HALF + (c + 1) * cut]], axis=1)
            for c in range(CHUNKS)
        ]
    kvs = [[chunk] + [behind(chunk, step) for step in range(1, reach + 1)] for chunk in chunks]
    results, parts = [], []
    for chunk in range(CHUNKS):
        made, pieces = attend(document_lengths, queries, gradient, kvs[chunk], chunk)
        results += made
        parts.append([pieces[0]] + [behind(pieces[step], -step) for step in range(1, reach + 1)])
    if by_hand:
        acc = None
        for chunk in range(CHUNKS):
            acc = finish(
                sizes, chunk, parts[chunk], acc and acc[0], mine + theirs, [] if chunk else results
            )
            if chunk == 0:
                attended, query_grad = acc[1:]
        input_grad = acc[0]
    else:
        sums = []
        for group in parts:
            total = group[0]
            for piece in group[1:]:
                total = total + piece.astype(jnp.float32)
            sums.append(total.astype(jnp.bfloat16))
        cut = CHUNK_HEADS * HEAD_SIZE
        flat = jnp.concatenate([s[:, :cut] for s in sums] + [s[:, cut:] for s in sums], axis=1)
        input_grad = lax.dot_general(flat, full, NT, preferred_element_type=jnp.float32).astype(jnp.bfloat16)
        attended = jnp.concatenate(results[0::2], axis=1)
        query_grad = jnp.concatenate(results[1::2], axis=1)
    return (attended[None], query_grad[None], input_grad[None])


def solution(mesh):
    sizes = (mesh.shape["dp"], mesh.shape["ctx"])
    return jax.shard_map(
        functools.partial(shards, sizes),
        mesh=mesh,
        in_specs=(
            P("dp", "ctx", None),
            P("dp", "ctx", None),
            P(("dp", "ctx"), None),
            P("dp", "ctx", None),
            P("dp", None),
        ),
        out_specs=(P("dp", "ctx", None), P("dp", "ctx", None), P("dp", "ctx", None)),
        check_vma=False,
    )
```

```python
import functools
import math

import jax
import jax.numpy as jnp
from jax import lax
from jax.experimental import pallas as pl
from jax.experimental.pallas import tpu as pltpu
from jax.sharding import PartitionSpec as P


QUERY_HEADS = 32
KEY_VALUE_HEADS = 4
HEAD_SIZE = 128
HEAD_GROUP = QUERY_HEADS // KEY_VALUE_HEADS
HALF = KEY_VALUE_HEADS * HEAD_SIZE
CHUNK_HEADS = 2
CHUNKS = KEY_VALUE_HEADS // CHUNK_HEADS
AXES = ("dp", "ctx")
NEGATIVE = -1e30


VMEM = pl.BlockSpec(memory_space=pltpu.VMEM)
SMEM = pl.BlockSpec(memory_space=pltpu.SMEM)
HBM = pl.BlockSpec(memory_space=pltpu.HBM)
NT = (((1,), (1,)), ((), ()))


def params(mib):
    return pltpu.CompilerParams(vmem_limit_bytes=mib * 1024 * 1024)


def cost(flops, moved):
    return pl.CostEstimate(flops=flops, bytes_accessed=moved, transcendentals=0)


def inside(value):
    return pltpu.with_memory_space_constraint(value, pltpu.VMEM)


def outside(value):
    return pltpu.with_memory_space_constraint(value, pltpu.HBM)


def columns(index):
    return pl.ds(pl.multiple_of(index * 128, 128), 128)


def shard_of(depth, across, core, block):
    z = lax.axis_index("dp")
    place = lax.axis_index("ctx")
    source = z - block // 4
    source = jnp.where(source < 0, source + depth, source)
    place = place - 2 * (place % 2) * core + core
    flip = block % 4
    if flip & 1:
        place = place + 2 - 4 * ((place // 2) % 2)
    if flip & 2:
        place = place + 4 - 8 * ((place // 4) % 2)
    return source * across + place


def arrange_kernel(sizes, x_ref, y_ref, out_ref):
    rows = x_ref.shape[0]
    for j in range(out_ref.shape[1] // 128):
        place = slice(j * 128, (j + 1) * 128)
        shard = shard_of(*sizes, 0, j)
        out_ref[:rows, place] = x_ref[:, columns(shard)]
        out_ref[rows:, place] = y_ref[:, columns(shard)]


def arrange(sizes, mine, other):
    rows, width = mine.shape
    return pl.pallas_call(
        functools.partial(arrange_kernel, sizes),
        out_shape=pltpu.VMEM((2 * rows, width // 2), mine.dtype),
        in_specs=[VMEM, VMEM],
        out_specs=VMEM,
        compiler_params=params(16),
        cost_estimate=cost(1 << 20, 3 << 20),
        name="arrange",
    )(mine, inside(other))


def fetch_kernel(count, *refs):
    sems = refs[-1]
    moves = [pltpu.make_async_copy(refs[j], refs[count + j], sems.at[j]) for j in range(count)]
    for move in moves:
        move.start()
    for move in moves:
        move.wait()


def fetch(*values):
    count = len(values)
    return pl.pallas_call(
        functools.partial(fetch_kernel, count),
        out_shape=[pltpu.VMEM(value.shape, value.dtype) for value in values],
        in_specs=[HBM] * count,
        out_specs=[VMEM] * count,
        scratch_shapes=[pltpu.SemaphoreType.DMA((count,))],
        compiler_params=params(16),
        cost_estimate=cost(1 << 20, 4 << 20),
        name="fetch",
    )(*[outside(value) for value in values])


def project_kernel(slot, count, last, x_ref, *refs):
    refs = list(refs)
    if slot:
        acc_ref = refs.pop(0)
    pieces = [refs.pop(0) for _ in range(count)]
    packed_ref = refs.pop(0)
    outs = refs
    rows = x_ref[:, slice(slot * 512, (slot + 1) * 512)]
    half = rows.shape[0] // 2
    for n in range(0, 2 * HALF, 256):
        side = 0 if n < HALF else 1
        cut = slice(n, n + 256)
        part = slice(n - side * HALF, n - side * HALF + 256)
        blocks = [ref[:, cut] for ref in pieces[:3]]
        blocks.append(pieces[3][:, cut] if count == 4 else pieces[3 + side][:, part])
        weight = jnp.concatenate(blocks, axis=0)
        packed_ref[:, cut] = weight
        total = jnp.dot(rows, weight, preferred_element_type=jnp.float32)
        if slot:
            total = total + acc_ref[:, cut]
        if last:
            outs[0][:, cut] = total[:half]
            outs[1][:, cut] = total[half:]
        else:
            outs[0][:, cut] = total


def project(slot, x, acc, pieces, last):
    rows = x.shape[0] // 2
    out = [pltpu.VMEM((rows, 2 * HALF), jnp.float32)] * 2
    if not last:
        out = [pltpu.VMEM((2 * rows, 2 * HALF), jnp.float32)]
    given = [inside(x)] + ([] if slot == 0 else [inside(acc)])
    given += list(pieces[:1] if slot == 0 else []) + [inside(piece) for piece in pieces[0 if slot else 1 :]]
    outs = pl.pallas_call(
        functools.partial(project_kernel, slot, len(pieces), last),
        out_shape=[pltpu.VMEM((512, 2 * HALF), jnp.bfloat16)] + out,
        in_specs=[VMEM] * len(given),
        out_specs=[VMEM] * (len(out) + 1),
        compiler_params=params(16),
        cost_estimate=cost(4 * rows * 512 * 2 * HALF, 4 << 20),
        name="project",
    )(*given)
    return outs[0], outs[1:]


def join_kernel(a_ref, b_ref, *outs):
    cut = CHUNK_HEADS * HEAD_SIZE
    for c, out in enumerate(outs):
        for side in range(2):
            span = slice(side * HALF + c * cut, side * HALF + (c + 1) * cut)
            out[:, side * cut : (side + 1) * cut] = (a_ref[:, span] + b_ref[:, span]).astype(out.dtype)


def join(mine, other):
    rows = mine.shape[0]
    return pl.pallas_call(
        join_kernel,
        out_shape=[pltpu.VMEM((rows, 2 * CHUNK_HEADS * HEAD_SIZE), jnp.bfloat16)] * CHUNKS,
        in_specs=[VMEM, VMEM],
        out_specs=[VMEM] * CHUNKS,
        compiler_params=params(16),
        cost_estimate=cost(1 << 20, 2 << 20),
        name="join",
    )(inside(mine), inside(other))


def attend_kernel(chunk, reach, lengths_ref, q_ref, g_ref, *refs):
    refs = list(refs)
    kv = [refs.pop(0) for _ in range(reach + 1)]
    o_ref, dq_ref = refs[0], refs[1]
    parts = refs[2 : 3 + reach]
    bias_ref, score_ref, press_ref, w_ref, p_ref, s_ref = refs[3 + reach :]
    rows = q_ref.shape[0]
    share = o_ref.shape[1]
    window = (reach + 1) * rows
    start = lax.axis_index("ctx") * rows
    key_pos = start - reach * rows + lax.broadcasted_iota(jnp.int32, (window, rows), 0)
    query_pos = start + lax.broadcasted_iota(jnp.int32, (8, rows), 1)
    key_doc = jnp.zeros((window, rows), jnp.int32)
    query_doc = jnp.zeros((8, rows), jnp.int32)
    end = jnp.int32(0)
    for document in range(lengths_ref.shape[1]):
        end = end + lengths_ref[0, document]
        key_doc = key_doc + (key_pos >= end).astype(jnp.int32)
        query_doc = query_doc + (query_pos >= end).astype(jnp.int32)
    allowed = (key_doc == query_doc[:1]) & (key_pos <= query_pos[:1]) & (key_pos >= 0)
    bias_ref[...] = jnp.where(allowed, 0.0, NEGATIVE)
    scale = 1.0 / math.sqrt(HEAD_SIZE)
    factor = scale * math.log2(math.e)
    size = HEAD_GROUP * rows
    for head in range(CHUNK_HEADS):
        k_cut = slice(head * HEAD_SIZE, (head + 1) * HEAD_SIZE)
        v_cut = slice((CHUNK_HEADS + head) * HEAD_SIZE, (CHUNK_HEADS + head + 1) * HEAD_SIZE)
        keys = jnp.concatenate([kv[reach - j][:, k_cut] for j in range(reach + 1)], axis=0)
        values = jnp.concatenate([kv[reach - j][:, v_cut] for j in range(reach + 1)], axis=0)
        keys_t = keys.T
        values_t = values.T
        base = head * HEAD_GROUP * HEAD_SIZE
        outs = [slice(base + j * HEAD_SIZE, base + (j + 1) * HEAD_SIZE) for j in range(HEAD_GROUP)]
        cuts = [slice(cut.start + chunk * share, cut.stop + chunk * share) for cut in outs]
        mine = slice(head * size, (head + 1) * size)
        q_all = jnp.concatenate([q_ref[:, cut] for cut in cuts], axis=0)
        g_all = jnp.concatenate([g_ref[:, cut] for cut in cuts], axis=0)
        score_ref[:, mine] = lax.dot_general(keys, q_all, NT, preferred_element_type=jnp.float32)
        press_ref[:, mine] = lax.dot_general(values, g_all, NT, preferred_element_type=jnp.float32)
        inverses = []
        for j in range(HEAD_GROUP):
            spot = slice(head * size + j * rows, head * size + (j + 1) * rows)
            score = score_ref[:, spot] + bias_ref[...]
            top = jnp.max(score, axis=0, keepdims=True)
            weight = jnp.exp2((score - top) * factor)
            inverse = 1.0 / jnp.sum(weight, axis=0, keepdims=True)
            inverses.append(inverse)
            w_ref[:, spot] = weight.astype(jnp.bfloat16)
            prob = weight * inverse
            p_ref[:, spot] = prob.astype(jnp.bfloat16)
            product = jnp.sum(prob * press_ref[:, spot], axis=0, keepdims=True)
            s_ref[:, spot] = (prob * (press_ref[:, spot] - product)).astype(jnp.bfloat16)
        mixed = jnp.dot(values_t, w_ref[:, mine], preferred_element_type=jnp.float32)
        mixed = (mixed * jnp.concatenate(inverses, axis=1)).astype(jnp.bfloat16)
        dq = jnp.dot(keys_t, s_ref[:, mine], preferred_element_type=jnp.float32)
        dq = (dq * scale).astype(jnp.bfloat16)
        for j, cut in enumerate(outs):
            o_ref[:, cut] = mixed[:, j * rows : (j + 1) * rows].T
            dq_ref[:, cut] = dq[:, j * rows : (j + 1) * rows].T
        for j in range(reach + 1):
            span = slice((reach - j) * rows, (reach - j + 1) * rows)
            dk = jnp.dot(s_ref[span, mine], q_all, preferred_element_type=jnp.float32) * scale
            dv = jnp.dot(p_ref[span, mine], g_all, preferred_element_type=jnp.float32)
            parts[j][:, k_cut] = dk.astype(parts[j].dtype)
            parts[j][:, v_cut] = dv.astype(parts[j].dtype)


def attend(lengths, queries, gradient, kv, chunk):
    rows, width = queries.shape
    reach = len(kv) - 1
    share = width // CHUNKS
    window = (reach + 1) * rows
    given = [lengths] + [inside(value) for value in (queries, gradient, *kv)]
    whole = pltpu.VMEM((rows, share), jnp.bfloat16)
    piece = (rows, 2 * CHUNK_HEADS * HEAD_SIZE)
    size = CHUNK_HEADS * HEAD_GROUP * rows
    outs = pl.pallas_call(
        functools.partial(attend_kernel, chunk, reach),
        out_shape=[whole, whole]
        + [pltpu.VMEM(piece, jnp.float32 if j % 2 == 0 else jnp.bfloat16) for j in range(reach + 1)],
        in_specs=[SMEM] + [VMEM] * (reach + 3),
        out_specs=[VMEM] * (reach + 3),
        scratch_shapes=[
            pltpu.VMEM((window, rows), jnp.float32),
            pltpu.VMEM((window, size), jnp.float32),
            pltpu.VMEM((window, size), jnp.float32),
            pltpu.VMEM((window, size), jnp.bfloat16),
            pltpu.VMEM((window, size), jnp.bfloat16),
            pltpu.VMEM((window, size), jnp.bfloat16),
        ],
        compiler_params=params(min(60, 14 + 14 * window * size // (1 << 20))),
        cost_estimate=cost(12 * rows * window * share * 2, 4 << 20),
        name="attend",
    )(*given)
    return outs[:2], outs[2:]


def combine_kernel(near_ref, swapped_ref, far_ref, here_ref, onward_ref):
    second = lax.axis_index("ctx") % 2 == 1
    swapped = swapped_ref[...].astype(jnp.float32)
    here_ref[...] = near_ref[...] + jnp.where(second, 0.0, swapped)
    onward_ref[...] = (far_ref[...].astype(jnp.float32) + jnp.where(second, swapped, 0.0)).astype(jnp.bfloat16)


def combine(near, swapped, far):
    return pl.pallas_call(
        combine_kernel,
        out_shape=[pltpu.VMEM(near.shape, jnp.float32), pltpu.VMEM(near.shape, jnp.bfloat16)],
        in_specs=[VMEM] * 3,
        out_specs=[VMEM] * 2,
        compiler_params=params(16),
        cost_estimate=cost(1 << 18, 1 << 20),
        name="combine",
    )(inside(near), inside(swapped), inside(far))


def finish_kernel(sizes, chunk, terms, slots, extra, *refs):
    refs = list(refs)
    parts = [refs.pop(0) for _ in range(terms)]
    if chunk:
        acc_ref = refs.pop(0)
    halves = [[refs.pop(0) for _ in range(slots)] for _ in range(2)]
    results = [refs.pop(0) for _ in range(extra)]
    out_ref = refs.pop(0)
    last = chunk + 1 == CHUNKS
    moves = []
    if extra:
        sems = refs.pop()
        for j, ref in enumerate(results):
            share = ref.shape[1]
            spot = slice((j // 2) * share, (j // 2 + 1) * share)
            moves.append(pltpu.make_async_copy(ref, refs[j % 2].at[:, spot], sems.at[j]))
            moves[-1].start()
    if last:
        staged_ref, out_sems = refs
    cut = CHUNK_HEADS * HEAD_SIZE
    total = parts[0][...]
    for part in parts[1:]:
        total = total + part[...].astype(jnp.float32)
    flat = total.astype(jnp.bfloat16)
    near_cut = slice(chunk * cut, (chunk + 1) * cut)
    far_cut = slice(HALF + chunk * cut, HALF + (chunk + 1) * cut)
    for block in range(4 * slots):
        span = slice((block % 4) * 128, (block % 4 + 1) * 128)
        pair = [half[block // 4] for half in halves]
        weight = jnp.concatenate([ref[span, near_cut] for ref in pair], axis=0)
        result = lax.dot_general(flat[:, :cut], weight, NT, preferred_element_type=jnp.float32)
        weight = jnp.concatenate([ref[span, far_cut] for ref in pair], axis=0)
        result = result + lax.dot_general(flat[:, cut:], weight, NT, preferred_element_type=jnp.float32)
        near = slice(block * 256, (block + 1) * 256)
        if chunk:
            result = result + acc_ref[:, near]
        if not last:
            out_ref[:, near] = result
            continue
        staged_ref[:, near] = result.astype(jnp.bfloat16)
        for core in range(2):
            shard = shard_of(*sizes, core, block)
            moves.append(
                pltpu.make_async_copy(
                    staged_ref.at[:, slice(block * 256 + core * 128, block * 256 + (core + 1) * 128)],
                    out_ref.at[:, columns(shard)],
                    out_sems.at[2 * block + core],
                )
            )
            moves[-1].start()
    for move in moves:
        move.wait()


def finish(sizes, chunk, parts, acc, halves, results):
    rows = parts[0].shape[0]
    slots = len(halves) // 2
    width = len(halves) * 512
    given = [inside(value) for value in list(parts) + ([acc] if chunk else []) + list(halves) + list(results)]
    out, specs = [pltpu.VMEM((rows, width), jnp.float32)], [VMEM]
    scratch = []
    if results:
        out += [pltpu.HBM((rows, width), jnp.bfloat16)] * 2
        specs += [HBM] * 2
        scratch = [pltpu.SemaphoreType.DMA((len(results),))]
    if chunk + 1 == CHUNKS:
        out[0], specs[0] = pltpu.HBM((rows, width), jnp.bfloat16), HBM
        scratch += [pltpu.VMEM((rows, width), jnp.bfloat16), pltpu.SemaphoreType.DMA((8 * slots,))]
    return pl.pallas_call(
        functools.partial(finish_kernel, sizes, chunk, len(parts), slots, len(results)),
        out_shape=out,
        in_specs=[VMEM] * len(given),
        out_specs=specs,
        scratch_shapes=scratch,
        compiler_params=params(16),
        cost_estimate=cost(2 * rows * width * 2 * HALF // CHUNKS, 10 << 20),
        name="finish",
    )(*given)


def shards(sizes, queries, layer_input, key_value_weight, output_gradient, document_lengths):
    depth, across = sizes
    inputs = layer_input[0]
    reach = across // 4

    queries, gradient = queries[0], output_gradient[0]

    def moved(value, target):
        pairs = []
        for a in range(depth):
            for b in range(across):
                to = target(a, b)
                if to is not None:
                    pairs.append((a * across + b, to[0] * across + to[1]))
        return lax.ppermute(value, AXES, pairs)

    def over_x(value):
        return moved(value, lambda a, b: (a, b ^ 2))

    def over_y(value):
        return moved(value, lambda a, b: (a, b ^ 4))

    def over_core(value):
        return moved(value, lambda a, b: (a, b ^ 1))

    def along(value, steps):
        return moved(value, lambda a, b: ((a + steps) % depth, b))

    def behind(value, steps):
        return moved(value, lambda a, b: (a, b + steps) if 0 <= b + steps < across else None)

    by_hand = across == 8 and depth > 2 and key_value_weight.shape[0] == 128
    if by_hand:
        own, last = key_value_weight, depth - 1
        held, acc, mine, theirs = own, None, [], []
        other = over_core(inputs)
        queries, gradient = fetch(queries, gradient)
        lined = arrange(sizes, inputs, other)
        for slot in range(depth):
            held = along(held, 1) if slot else own
            if slot == last:
                rx, ry = along(side_x, slot), along(side_y, slot)
            else:
                rx, ry = over_x(held), over_y(held)
            if slot == 0:
                side_x, side_y = rx, ry
            pieces = [held, rx, ry]
            if slot == last:
                pieces += [over_y(rx)]
            elif slot == last - 1:
                pieces += [over_x(ry)]
            else:
                pieces += [over_y(rx[:, :HALF]), over_x(ry[:, HALF:])]
            packed, acc = project(slot, lined, acc, pieces, slot + 1 == depth)
            mine.append(packed)
            theirs.append(over_core(packed))
            if slot + 1 < depth:
                acc = acc[0]
        got = over_core(acc[1])
        chunks = join(acc[0], got)
    else:
        full = lax.all_gather(key_value_weight, AXES, axis=0, tiled=True)
        flat = jnp.dot(inputs, full, preferred_element_type=jnp.float32).astype(jnp.bfloat16)
        cut = CHUNK_HEADS * HEAD_SIZE
        chunks = [
            jnp.concatenate([flat[:, c * cut : (c + 1) * cut], flat[:, HALF + c * cut : HALF + (c + 1) * cut]], axis=1)
            for c in range(CHUNKS)
        ]
    kvs = [[chunk] + [behind(chunk, step) for step in range(1, reach + 1)] for chunk in chunks]
    results, parts = [], []
    for chunk in range(CHUNKS):
        made, pieces = attend(document_lengths, queries, gradient, kvs[chunk], chunk)
        results += made
        if by_hand:
            swapped = over_core(pieces[1])
            here, onward = combine(pieces[0], swapped, pieces[2])
            parts.append([here, behind(onward, -2)])
        else:
            parts.append([pieces[0]] + [behind(pieces[step], -step) for step in range(1, reach + 1)])
    if by_hand:
        acc = None
        for chunk in range(CHUNKS):
            acc = finish(
                sizes, chunk, parts[chunk], acc and acc[0], mine + theirs, [] if chunk else results
            )
            if chunk == 0:
                attended, query_grad = acc[1:]
        input_grad = acc[0]
    else:
        sums = []
        for group in parts:
            total = group[0]
            for piece in group[1:]:
                total = total + piece.astype(jnp.float32)
            sums.append(total.astype(jnp.bfloat16))
        cut = CHUNK_HEADS * HEAD_SIZE
        flat = jnp.concatenate([s[:, :cut] for s in sums] + [s[:, cut:] for s in sums], axis=1)
        input_grad = lax.dot_general(flat, full, NT, preferred_element_type=jnp.float32).astype(jnp.bfloat16)
        attended = jnp.concatenate(results[0::2], axis=1)
        query_grad = jnp.concatenate(results[1::2], axis=1)
    return (attended[None], query_grad[None], input_grad[None])


def solution(mesh):
    sizes = (mesh.shape["dp"], mesh.shape["ctx"])
    return jax.shard_map(
        functools.partial(shards, sizes),
        mesh=mesh,
        in_specs=(
            P("dp", "ctx", None),
            P("dp", "ctx", None),
            P(("dp", "ctx"), None),
            P("dp", "ctx", None),
            P("dp", None),
        ),
        out_specs=(P("dp", "ctx", None), P("dp", "ctx", None), P("dp", "ctx", None)),
        check_vma=False,
    )
```
